32 devices in a mesh: dp: 16 (over z, x, core), ens: 2 (over y).
Axes of the slice: x: 2, y: 2, z: 4, core: 2. Of those that a mesh axis runs over, the one named last changes fastest.
Arguments:
- embeddings: bfloat16 [12288, 1024], P('dp'), may hold values from -6 to 6
- valid_mask: int32 [12288], P('dp'), may hold values 0 or 1
- first_weight: bfloat16 [2, 1024, 4096], P(None, 'dp', 'ens'), may hold values from -0.1875 to 0.1875
- second_weight: bfloat16 [2, 4096, 128], P(None, 'ens'), may hold values from -0.09375 to 0.09375
- thresholds: int32 [2], replicated, may hold values from -256 to 256
Outputs:
- mean_logits: float32 [12288, 128], P('dp')
- kept_share: float32 [2], P('ens')
- agree_share: float32 [2], P('ens')
The draws below stay inside these ranges and needn't reach their ends.
All inputs are finite; a program needn't handle non-finite values. No bound on the sum of `valid_mask` on one device may be relied on, other than what follows from the above.
Results may differ from the reference program's by a relative error of at most 0.0044.
Values may be sent and summed in bfloat16 or wider, within the bound.
A program may use at most 64 MiB of HBM per device.

```python
import jax
import jax.numpy as jnp
from jax import lax

D = 1024
H = 4096
C = 128
DOC_DEV = 768
MEMBERS = 2
DOCS = 12288
N_DP = 16


def with_ends(array, stream_key, low, largest):
    index_at = [jax.random.randint(jax.random.fold_in(stream_key, axis), (), 0, length) for axis, length in enumerate(array.shape)]
    widest = array.shape.index(max(array.shape))
    next_to = index_at[:widest] + [(index_at[widest] + 1) % array.shape[widest]] + index_at[widest + 1:]
    return array.at[tuple(index_at)].set(low).at[tuple(next_to)].set(largest)


def block_scale(own_key, extent, split, least, high):
    loudness = 1.0
    for position, blocks in split:
        heights = jax.random.uniform(jax.random.fold_in(jax.random.fold_in(own_key, 6), position), (blocks,), jnp.float32, least / len(split), high / len(split))
        loudness = loudness * jnp.repeat(jnp.exp(heights), extent[position] // blocks).reshape((-1,) + (1,) * (len(extent) - 1 - position))
    return loudness


def noise(own_key, dims, scale, reach, pieces=(), kind=jnp.bfloat16):
    entries = jax.random.normal(own_key, dims, jnp.float32) * scale
    if len(pieces) > 0:
        entries = block_scale(own_key, dims, pieces, -0.22, 0.18) * entries
    return jnp.clip(entries, min=-reach, max=reach).astype(kind)


def setup_inputs(seed: int = 0) -> dict:
    seeds = jax.random.split(jax.random.key(seed), 6)
    return {
        "embeddings": noise(seeds[0], (DOCS, D), 1.0, 6.0, ((0, 16),)),
        "valid_mask": with_ends((jax.random.randint(seeds[1], (DOCS,), 0, 4) < 3).astype(jnp.int32), jax.random.fold_in(seeds[1], 1), 0, 1),
        "first_weight": noise(seeds[2], (MEMBERS, D, H), D ** -0.5, 0.1875, ((1, 16), (2, 2))),
        "second_weight": noise(seeds[3], (MEMBERS, H, C), H ** -0.5, 0.09375, ((1, 2),)),
        "thresholds": jax.random.randint(seeds[4], (MEMBERS,), -256, 257).astype(jnp.int32),
    }


def member_logits(embeddings, first_weight, second_weight):
    blocks = embeddings.reshape(N_DP, DOC_DEV, D)

    def one_member(weights):
        layer_one, layer_two = weights

        def one_block(block_rows):
            hidden = jnp.maximum(jnp.dot(block_rows, layer_one, preferred_element_type=jnp.float32), 0.0).astype(jnp.bfloat16)
            return jnp.dot(hidden, layer_two, preferred_element_type=jnp.float32)
        return lax.map(one_block, blocks).reshape(DOCS, C)
    return lax.map(one_member, (first_weight, second_weight))

def reference(embeddings, valid_mask, first_weight, second_weight, thresholds):
    logits = member_logits(embeddings, first_weight, second_weight)
    mean_logits = lax.optimization_barrier(jnp.sum(logits, axis=0)) / MEMBERS
    levels = jnp.arange(C, dtype=jnp.float32)
    grades = (2.0 * levels / (C - 1) - 1.0) * jnp.sqrt(jnp.float32(3.0 / C))
    scores = jnp.einsum('edc,c->ed', logits, grades, precision=lax.Precision.HIGHEST)
    ens_score = jnp.dot(mean_logits, grades, precision=lax.Precision.HIGHEST)
    cutoffs = thresholds.astype(jnp.float32) / 256.0
    validity = valid_mask.astype(jnp.float32)
    kept_soft = validity[None, :] * jax.nn.sigmoid(4.0 * (scores - cutoffs[:, None]))
    ens_kept = jax.nn.sigmoid(4.0 * (ens_score - jnp.mean(cutoffs)))
    kept_share = lax.optimization_barrier(jnp.sum(kept_soft, axis=1)) / DOC_DEV
    agree_share = lax.optimization_barrier(jnp.sum(kept_soft * ens_kept[None, :], axis=1)) / DOC_DEV
    return (mean_logits, kept_share, agree_share)
```

```python
import jax
import jax.numpy as jnp
from jax import lax
from jax.sharding import PartitionSpec as P


def on_device(embeddings, valid_mask, first_weight, second_weight, thresholds):
    members, rows, units = first_weight.shape
    member = lax.axis_index("ens")
    own = members // lax.axis_size("ens")
    full_first = lax.all_gather(first_weight, "dp", axis=1, tiled=True)
    partial = []
    for m in range(members):
        hidden = jnp.maximum(
            jnp.dot(embeddings, full_first[m], preferred_element_type=jnp.float32), 0.0
        ).astype(jnp.bfloat16)
        partial.append(jnp.dot(hidden, second_weight[m], preferred_element_type=jnp.float32))
    classes = partial[0].shape[1]
    levels = jnp.arange(classes, dtype=jnp.float32)
    grades = (2.0 * levels / (classes - 1) - 1.0) * jnp.sqrt(jnp.float32(3.0 / classes))
    scores = jnp.stack([jnp.dot(p, grades, precision=lax.Precision.HIGHEST) for p in partial])
    mean_logits, scores = lax.psum((sum(partial) / members, scores), "ens")
    cutoffs = thresholds.astype(jnp.float32) / 256.0
    own_scores = lax.dynamic_slice_in_dim(scores, member * own, own, 0)
    own_cutoffs = lax.dynamic_slice_in_dim(cutoffs, member * own, own, 0)
    validity = valid_mask.astype(jnp.float32)
    kept = validity * jax.nn.sigmoid(4.0 * (own_scores - own_cutoffs[:, None]))
    ens_kept = jax.nn.sigmoid(4.0 * (jnp.mean(scores, axis=0) - jnp.mean(cutoffs)))
    sums = jnp.stack([jnp.sum(kept, axis=1), jnp.sum(kept * ens_kept, axis=1)])
    sums = lax.psum(sums, "dp") / embeddings.shape[0]
    return mean_logits, sums[0], sums[1]


def solution(mesh):
    return jax.shard_map(
        on_device,
        mesh=mesh,
        in_specs=(P("dp", None), P("dp"), P(None, "dp", "ens"), P(None, "ens", None), P()),
        out_specs=(P("dp", None), P("ens"), P("ens")),
        check_vma=False,
    )
```

```python
import functools

import jax
import jax.numpy as jnp
from jax import lax
from jax.experimental import pallas as pl
from jax.experimental.pallas import tpu as pltpu
from jax.sharding import PartitionSpec as P

MESH = pl.DeviceIdType.MESH
COLS = 256
LAG = 1
PARTS = 2


def geometry(mesh):
    line = [tuple(d.coords) for d in mesh.devices.reshape(mesh.devices.shape[0], -1)[:, 0]]
    cores = sum(c == line[0] for c in line)
    chips = line[::cores]
    inner = 1
    if len(chips) > 1:
        axis = [a != b for a, b in zip(chips[0], chips[1])].index(True)
        while inner < len(chips) and chips[inner][axis] == chips[0][axis] + inner:
            inner += 1
    return len(chips) // inner, inner, cores


def turned_period(nz, nx):
    even = (nz - 1) * nx - (nx - 1)
    slope = (nz - 1) * (nx - 1) + (nz - 1) * (nx - 1)
    share = 1.0 - even / slope if slope else 0.0
    return round(1 / share) if share > 0 else 0


def kernel(
    geo, n_ens, emb_hbm, mask_ref, fw_hbm, sw_hbm, thr_ref, out_ref, kept_ref, agree_ref,
    w, emb, sw, acc, part, sc, tot,
    local_sem, emb_sem, send_sem, recv_sem, part_send, part_recv, sc_send, sc_recv, tot_send, tot_recv,
):
    nz, nx, nc = geo
    n_dp = nz * nx * nc
    n_chips = nz * nx
    members, rows, units = fw_hbm.shape
    per_member = units // COLS
    chunks = members * per_member
    docs, classes = out_ref.shape
    period = turned_period(nz, nx)
    reach = nz - 1 + nx - 1
    slots = send_sem.shape[0]

    me = lax.axis_index("dp")
    ens = lax.axis_index("ens")
    core = lax.rem(me, nc)
    chip = me // nc
    z, x = chip // nx, lax.rem(chip, nx)

    def origin_rows(origin):
        return pl.ds(pl.multiple_of(origin * rows, rows), rows)

    def own_copy(c):
        cols = pl.ds(pl.multiple_of(lax.rem(c, per_member) * COLS, COLS), COLS)
        return pltpu.make_async_copy(
            fw_hbm.at[c // per_member, :, cols], w.at[c, origin_rows(me), :], local_sem.at[c]
        )

    for c in range(chunks):
        own_copy(jnp.int32(c)).start()
    emb_copy = pltpu.make_async_copy(emb_hbm, emb, emb_sem.at[0])
    sw_copy = pltpu.make_async_copy(sw_hbm, sw, emb_sem.at[1])
    emb_copy.start()
    sw_copy.start()

    barrier = pltpu.get_barrier_semaphore()
    dirs = []
    if nz > 1:
        dirs += [("z", 1), ("z", -1)]
    if nx > 1:
        dirs += [("x", 1), ("x", -1)]
    dirs += [("c", k) for k in range(1, nc)]

    def target(d):
        kind, k = d
        if kind == "z":
            return me + k * nx * nc
        if kind == "x":
            return me + k * nc
        return chip * nc + lax.rem(core + k, nc)

    def there(d):
        kind, k = d
        if kind == "c":
            return None
        at, n = (z, nz) if kind == "z" else (x, nx)
        return at + 1 < n if k > 0 else at > 0

    waits = jnp.int32(nc - 1 + n_ens - 1)
    for d in dirs:
        ok = there(d)
        if ok is None:
            pl.semaphore_signal(barrier, inc=1, device_id={"dp": target(d)}, device_id_type=MESH)
        else:
            @pl.when(ok)
            def _():
                pl.semaphore_signal(barrier, inc=1, device_id={"dp": target(d)}, device_id_type=MESH)
            waits = waits + ok.astype(jnp.int32)
    for k in range(1, n_ens):
        pl.semaphore_signal(
            barrier, inc=1, device_id={"ens": lax.rem(ens + k, n_ens)}, device_id_type=MESH
        )
    pl.semaphore_wait(barrier, waits)

    def turned(c):
        if not period:
            return jnp.bool_(False)
        return lax.rem(c, period) == period // 2

    def goes(d, c, zo, xo):
        kind, k = d
        if kind == "c":
            return c >= 0
        inner_first = turned(c)
        if kind == "z":
            away = (z >= zo) if k > 0 else (z <= zo)
            return away & there(d) & ((xo == x) | inner_first)
        away = (x >= xo) if k > 0 else (x <= xo)
        return away & there(d) & ((zo == z) | jnp.logical_not(inner_first))

    def sending(i, d, c, zo, xo):
        place = zo * nx + xo
        origin = place * nc + core
        block = w.at[c, origin_rows(origin), :]
        return pltpu.make_async_remote_copy(
            src_ref=block, dst_ref=block,
            send_sem=send_sem.at[lax.rem(c, slots), i, place], recv_sem=recv_sem.at[c, origin],
            device_id={"dp": target(d)}, device_id_type=MESH,
        )

    def arrived(c, origin):
        block = w.at[c, origin_rows(origin), :]
        pltpu.make_async_remote_copy(
            src_ref=block, dst_ref=block, send_sem=send_sem.at[0, 0, 0], recv_sem=recv_sem.at[c, origin],
            device_id={"dp": target(dirs[-1])}, device_id_type=MESH,
        ).wait_recv()

    def place_of(k):
        kz, kx = divmod(k, nx)
        return lax.rem(z + kz, nz), lax.rem(x + kx, nx)

    acc[...] = jnp.zeros_like(acc)

    def step(t, carry):
        for k in range(n_chips):
            zo, xo = place_of(k)
            c = t - LAG * (jnp.abs(z - zo) + jnp.abs(x - xo))

            @pl.when((c >= 0) & (c < chunks))
            def _():
                if k == 0:
                    own_copy(c).wait()
                else:
                    arrived(c, (zo * nx + xo) * nc + core)
                for i, d in enumerate(dirs):
                    @pl.when((c >= slots) & goes(d, c - slots, zo, xo))
                    def _():
                        sending(i, d, c - slots, zo, xo).wait_send()

                    @pl.when(goes(d, c, zo, xo))
                    def _():
                        sending(i, d, c, zo, xo).start()

        done = t - LAG * reach - 1

        @pl.when(done >= 0)
        def _():
            @pl.when(done == 0)
            def _():
                emb_copy.wait()
                sw_copy.wait()
            for k in range(n_chips):
                for o in range(1, nc):
                    arrived(done, k * nc + lax.rem(core + o, nc))
            m = done // per_member
            cols = pl.ds(pl.multiple_of(lax.rem(done, per_member) * COLS, COLS), COLS)
            hidden = jnp.maximum(
                jnp.dot(emb[...], w[done], preferred_element_type=jnp.float32), 0.0
            ).astype(jnp.bfloat16)
            acc[m] += jnp.dot(hidden, sw[m, cols, :], preferred_element_type=jnp.float32)
        return carry

    lax.fori_loop(0, chunks + LAG * reach + 1, step, 0)

    lines = sc.shape[1]
    levels = lax.broadcasted_iota(jnp.int32, (lines, classes), 1).astype(jnp.float32)
    grades = (2.0 * levels / (classes - 1) - 1.0) * jnp.sqrt(jnp.float32(3.0 / classes))
    line = lax.broadcasted_iota(jnp.int32, (lines, classes), 0)
    own_scores = jnp.zeros((lines, docs), jnp.float32)
    for m in range(members):
        own_scores += lax.dot_general(
            jnp.where(line == m, grades, 0.0), acc[m], (((1,), (1,)), ((), ())),
            precision=lax.Precision.HIGHEST, preferred_element_type=jnp.float32,
        )
    sc[ens] = own_scores

    def sc_copy(k):
        return pltpu.make_async_remote_copy(
            src_ref=sc.at[ens], dst_ref=sc.at[ens], send_sem=sc_send.at[k], recv_sem=sc_recv.at[ens],
            device_id={"ens": lax.rem(ens + k, n_ens)}, device_id_type=MESH,
        )

    def part_copy(k, b):
        piece = part.at[ens, pl.ds(b * (docs // PARTS), docs // PARTS), :]
        return pltpu.make_async_remote_copy(
            src_ref=piece, dst_ref=piece, send_sem=part_send.at[k, b], recv_sem=part_recv.at[ens, b],
            device_id={"ens": lax.rem(ens + k, n_ens)}, device_id_type=MESH,
        )

    for k in range(1, n_ens):
        sc_copy(k).start()
    for b in range(PARTS):
        piece = pl.ds(b * (docs // PARTS), docs // PARTS)
        total = acc[0, piece, :]
        for m in range(1, members):
            total += acc[m, piece, :]
        part[ens, piece, :] = (total * (1.0 / members)).astype(jnp.bfloat16)
        for k in range(1, n_ens):
            part_copy(k, b).start()

    for k in range(1, n_ens):
        other = lax.rem(ens + k, n_ens)
        pltpu.make_async_remote_copy(
            src_ref=sc.at[other], dst_ref=sc.at[other], send_sem=sc_send.at[k], recv_sem=sc_recv.at[other],
            device_id={"ens": other}, device_id_type=MESH,
        ).wait_recv()
    scores = sc[0]
    for k in range(1, n_ens):
        scores += sc[k]
    row = lax.broadcasted_iota(jnp.int32, (lines, docs), 0)
    cutoff = jnp.zeros((lines, docs), jnp.float32)
    mean_cutoff = jnp.float32(0.0)
    for m in range(members):
        level = thr_ref[m].astype(jnp.float32) * (1.0 / 256.0)
        cutoff = jnp.where(row == m, level, cutoff)
        mean_cutoff += level * (1.0 / members)
    kept = mask_ref[...].astype(jnp.float32) * jax.nn.sigmoid(4.0 * (scores - cutoff))
    ens_score = jnp.sum(scores, axis=0, keepdims=True) * (1.0 / members)
    ens_kept = jax.nn.sigmoid(4.0 * (ens_score - mean_cutoff))
    kept_sum = jnp.sum(kept, axis=1, keepdims=True)
    agree_sum = jnp.sum(kept * ens_kept, axis=1, keepdims=True)
    lane = lax.broadcasted_iota(jnp.int32, (lines, 128), 1)
    tot[me] = jnp.where(lane == 0, kept_sum, jnp.where(lane == 1, agree_sum, 0.0))

    def tot_copy(k):
        return pltpu.make_async_remote_copy(
            src_ref=tot.at[me], dst_ref=tot.at[me], send_sem=tot_send.at[k], recv_sem=tot_recv.at[me],
            device_id={"dp": lax.rem(me + k, n_dp)}, device_id_type=MESH,
        )

    for k in range(1, n_dp):
        tot_copy(k).start()

    for b in range(PARTS):
        piece = pl.ds(b * (docs // PARTS), docs // PARTS)
        for k in range(1, n_ens):
            other = lax.rem(ens + k, n_ens)
            block = part.at[other, piece, :]
            pltpu.make_async_remote_copy(
                src_ref=block, dst_ref=block, send_sem=part_send.at[k, b], recv_sem=part_recv.at[other, b],
                device_id={"ens": other}, device_id_type=MESH,
            ).wait_recv()
        total = part[0, piece, :].astype(jnp.float32)
        for k in range(1, n_ens):
            total += part[k, piece, :].astype(jnp.float32)
        out_ref[piece, :] = total

    for k in range(1, n_dp):
        other = lax.rem(me + k, n_dp)
        pltpu.make_async_remote_copy(
            src_ref=tot.at[other], dst_ref=tot.at[other], send_sem=tot_send.at[k], recv_sem=tot_recv.at[other],
            device_id={"dp": other}, device_id_type=MESH,
        ).wait_recv()
    sums = tot[0]
    for k in range(1, n_dp):
        sums += tot[k]
    sums = sums / docs
    own = members // n_ens
    row = lax.broadcasted_iota(jnp.int32, (lines, 128), 0)
    for j in range(own):
        mine = row == ens * own + j
        kept_ref[j] = jnp.sum(jnp.where(mine & (lane == 0), sums, 0.0))
        agree_ref[j] = jnp.sum(jnp.where(mine & (lane == 1), sums, 0.0))

    for k in range(n_chips):
        zo, xo = place_of(k)
        for c in range(max(0, chunks - slots), chunks):
            for i, d in enumerate(dirs):
                @pl.when(goes(d, jnp.int32(c), zo, xo))
                def _():
                    sending(i, d, jnp.int32(c), zo, xo).wait_send()
    for k in range(1, n_ens):
        sc_copy(k).wait_send()
        for b in range(PARTS):
            part_copy(k, b).wait_send()
    for k in range(1, n_dp):
        tot_copy(k).wait_send()


def solution(mesh):
    geo = geometry(mesh)
    nz, nx, nc = geo
    n_dp, n_ens = mesh.shape["dp"], mesh.shape["ens"]

    def on_device(embeddings, valid_mask, first_weight, second_weight, thresholds):
        docs, width = embeddings.shape
        members, rows, units = first_weight.shape
        classes = second_weight.shape[2]
        chunks = members * units // COLS
        own = members // n_ens
        lines = -(-members // 8) * 8
        dma = pltpu.SemaphoreType.DMA
        hbm, vmem, smem = (pl.BlockSpec(memory_space=s) for s in (pl.ANY, pltpu.VMEM, pltpu.SMEM))
        return pl.pallas_call(
            functools.partial(kernel, geo, n_ens),
            out_shape=(
                jax.ShapeDtypeStruct((docs, classes), jnp.float32),
                jax.ShapeDtypeStruct((own,), jnp.float32),
                jax.ShapeDtypeStruct((own,), jnp.float32),
            ),
            in_specs=[hbm, vmem, hbm, hbm, smem],
            out_specs=(vmem, smem, smem),
            scratch_shapes=[
                pltpu.VMEM((chunks, width, COLS), jnp.bfloat16),
                pltpu.VMEM((docs, width), jnp.bfloat16),
                pltpu.VMEM(second_weight.shape, jnp.bfloat16),
                pltpu.VMEM((members, docs, classes), jnp.float32),
                pltpu.VMEM((n_ens, docs, classes), jnp.bfloat16),
                pltpu.VMEM((n_ens, lines, docs), jnp.float32),
                pltpu.VMEM((n_dp, lines, 128), jnp.float32),
                dma((chunks,)),
                dma((2,)),
                dma((2, 4 + nc - 1, nz * nx)),
                dma((chunks, n_dp)),
                dma((n_ens, PARTS)),
                dma((n_ens, PARTS)),
                dma((n_ens,)),
                dma((n_ens,)),
                dma((n_dp,)),
                dma((n_dp,)),
            ],
            compiler_params=pltpu.CompilerParams(
                collective_id=0, has_side_effects=True, vmem_limit_bytes=48 * 1024 * 1024
            ),
        )(embeddings, valid_mask.reshape(1, docs), first_weight, second_weight, thresholds)

    return jax.shard_map(
        on_device,
        mesh=mesh,
        in_specs=(P("dp", None), P("dp"), P(None, "dp", "ens"), P(None, "ens", None), P()),
        out_specs=(P("dp", None), P("ens"), P("ens")),
        check_vma=False,
    )
```

```python
import functools

import jax
import jax.numpy as jnp
from jax import lax
from jax.experimental import pallas as pl
from jax.experimental.pallas import tpu as pltpu
from jax.sharding import PartitionSpec as P

MESH = pl.DeviceIdType.MESH
COLS = 512
LAG = 2
PARTS = 2
SLOTS = 2


def geometry(mesh):
    line = [tuple(d.coords) for d in mesh.devices.reshape(mesh.devices.shape[0], -1)[:, 0]]
    cores = sum(c == line[0] for c in line)
    chips = line[::cores]
    inner = 1
    if len(chips) > 1:
        axis = [a != b for a, b in zip(chips[0], chips[1])].index(True)
        while inner < len(chips) and chips[inner][axis] == chips[0][axis] + inner:
            inner += 1
    return len(chips) // inner, inner, cores


def turned_period(nz, nx):
    even = (nz - 1) * nx - (nx - 1)
    slope = (nz - 1) * (nx - 1) + (nz - 1) * (nx - 1)
    share = 1.0 - even / slope if slope else 0.0
    return round(1 / share) if share > 0 else 0


def kernel(
    geo, n_ens, emb_hbm, mask_ref, fw_hbm, sw_hbm, thr_ref, out_ref, kept_ref, agree_ref,
    w, emb, sw, acc, part, sc, tot,
    local_sem, emb_sem, send_sem, recv_sem, part_send, part_recv, sc_send, sc_recv, tot_send, tot_recv,
):
    nz, nx, nc = geo
    n_dp = nz * nx * nc
    n_chips = nz * nx
    members, rows, units = fw_hbm.shape
    per_member = units // COLS
    chunks = members * per_member
    docs, classes = out_ref.shape
    period = turned_period(nz, nx)
    reach = nz - 1 + nx - 1
    slots = send_sem.shape[0]

    me = lax.axis_index("dp")
    ens = lax.axis_index("ens")
    core = lax.rem(me, nc)
    chip = me // nc
    z, x = chip // nx, lax.rem(chip, nx)

    def origin_rows(origin):
        return pl.ds(pl.multiple_of(origin * rows, rows), rows)

    def own_copy(c):
        cols = pl.ds(pl.multiple_of(lax.rem(c, per_member) * COLS, COLS), COLS)
        return pltpu.make_async_copy(
            fw_hbm.at[c // per_member, :, cols], w.at[c, origin_rows(me), :], local_sem.at[c]
        )

    for c in range(chunks):
        own_copy(jnp.int32(c)).start()
    emb_copy = pltpu.make_async_copy(emb_hbm, emb, emb_sem.at[0])
    sw_copy = pltpu.make_async_copy(sw_hbm, sw, emb_sem.at[1])
    emb_copy.start()
    sw_copy.start()

    barrier = pltpu.get_barrier_semaphore()
    dirs = []
    if nz > 1:
        dirs += [("z", 1), ("z", -1)]
    if nx > 1:
        dirs += [("x", 1), ("x", -1)]
    dirs += [("c", k) for k in range(1, nc)]

    def target(d):
        kind, k = d
        if kind == "z":
            return me + k * nx * nc
        if kind == "x":
            return me + k * nc
        return chip * nc + lax.rem(core + k, nc)

    def there(d):
        kind, k = d
        if kind == "c":
            return None
        at, n = (z, nz) if kind == "z" else (x, nx)
        return at + 1 < n if k > 0 else at > 0

    waits = jnp.int32(nc - 1 + n_ens - 1)
    for d in dirs:
        ok = there(d)
        if ok is None:
            pl.semaphore_signal(barrier, inc=1, device_id={"dp": target(d)}, device_id_type=MESH)
        else:
            @pl.when(ok)
            def _():
                pl.semaphore_signal(barrier, inc=1, device_id={"dp": target(d)}, device_id_type=MESH)
            waits = waits + ok.astype(jnp.int32)
    for k in range(1, n_ens):
        pl.semaphore_signal(
            barrier, inc=1, device_id={"ens": lax.rem(ens + k, n_ens)}, device_id_type=MESH
        )
    pl.semaphore_wait(barrier, waits)

    def turned(c):
        if not period:
            return jnp.bool_(False)
        return lax.rem(c * nc + core, period) == period // 2

    def goes(d, c, zo, xo):
        kind, k = d
        if kind == "c":
            return c >= 0
        inner_first = turned(c)
        if kind == "z":
            away = (z >= zo) if k > 0 else (z <= zo)
            return away & there(d) & ((xo == x) | inner_first)
        away = (x >= xo) if k > 0 else (x <= xo)
        return away & there(d) & ((zo == z) | jnp.logical_not(inner_first))

    def sending(i, d, c, zo, xo):
        place = zo * nx + xo
        origin = place * nc + core
        block = w.at[c, origin_rows(origin), :]
        return pltpu.make_async_remote_copy(
            src_ref=block, dst_ref=block,
            send_sem=send_sem.at[lax.rem(c, slots), i, place], recv_sem=recv_sem.at[c, origin],
            device_id={"dp": target(d)}, device_id_type=MESH,
        )

    def arrived(c, origin):
        block = w.at[c, origin_rows(origin), :]
        pltpu.make_async_remote_copy(
            src_ref=block, dst_ref=block, send_sem=send_sem.at[0, 0, 0], recv_sem=recv_sem.at[c, origin],
            device_id={"dp": target(dirs[-1])}, device_id_type=MESH,
        ).wait_recv()

    def place_of(k):
        kz, kx = divmod(k, nx)
        return lax.rem(z + kz, nz), lax.rem(x + kx, nx)

    acc[...] = jnp.zeros_like(acc)

    def compute(done):
        @pl.when(done >= 0)
        def _():
            @pl.when(done == 0)
            def _():
                emb_copy.wait()
                sw_copy.wait()
            for k in range(n_chips):
                for o in range(1, nc):
                    arrived(done, k * nc + lax.rem(core + o, nc))
            m = done // per_member
            cols = pl.ds(pl.multiple_of(lax.rem(done, per_member) * COLS, COLS), COLS)
            hidden = jnp.maximum(
                jnp.dot(emb[...], w[done], preferred_element_type=jnp.float32), 0.0
            ).astype(jnp.bfloat16)
            acc[m] += jnp.dot(hidden, sw[m, cols, :], preferred_element_type=jnp.float32)

    def step(t, carry):
        for k in range(n_chips):
            zo, xo = place_of(k)
            c = t - LAG * (jnp.abs(z - zo) + jnp.abs(x - xo))

            @pl.when((c >= 0) & (c < chunks))
            def _():
                if k == 0:
                    own_copy(c).wait()
                else:
                    arrived(c, (zo * nx + xo) * nc + core)
                for i, d in enumerate(dirs):
                    @pl.when((c >= slots) & goes(d, c - slots, zo, xo))
                    def _():
                        sending(i, d, c - slots, zo, xo).wait_send()

                    @pl.when(goes(d, c, zo, xo))
                    def _():
                        sending(i, d, c, zo, xo).start()

            if k == n_chips - 1:
                compute(t - LAG * reach - 1)
        return carry

    lax.fori_loop(0, chunks + LAG * reach + 1, step, 0)

    lines = sc.shape[1]
    levels = lax.broadcasted_iota(jnp.int32, (lines, classes), 1).astype(jnp.float32)
    grades = (2.0 * levels / (classes - 1) - 1.0) * jnp.sqrt(jnp.float32(3.0 / classes))
    line = lax.broadcasted_iota(jnp.int32, (lines, classes), 0)
    own_scores = jnp.zeros((lines, docs), jnp.float32)
    for m in range(members):
        own_scores += lax.dot_general(
            jnp.where(line == m, grades, 0.0), acc[m], (((1,), (1,)), ((), ())),
            precision=lax.Precision.HIGHEST, preferred_element_type=jnp.float32,
        )
    sc[ens] = own_scores

    def sc_copy(k):
        return pltpu.make_async_remote_copy(
            src_ref=sc.at[ens], dst_ref=sc.at[ens], send_sem=sc_send.at[k], recv_sem=sc_recv.at[ens],
            device_id={"ens": lax.rem(ens + k, n_ens)}, device_id_type=MESH,
        )

    def part_copy(k, b):
        piece = part.at[ens, pl.ds(b * (docs // PARTS), docs // PARTS), :]
        return pltpu.make_async_remote_copy(
            src_ref=piece, dst_ref=piece, send_sem=part_send.at[k, b], recv_sem=part_recv.at[ens, b],
            device_id={"ens": lax.rem(ens + k, n_ens)}, device_id_type=MESH,
        )

    for k in range(1, n_ens):
        sc_copy(k).start()
    for b in range(PARTS):
        piece = pl.ds(b * (docs // PARTS), docs // PARTS)
        total = acc[0, piece, :]
        for m in range(1, members):
            total += acc[m, piece, :]
        part[ens, piece, :] = (total * (1.0 / members)).astype(jnp.bfloat16)
        for k in range(1, n_ens):
            part_copy(k, b).start()

    for k in range(1, n_ens):
        other = lax.rem(ens + k, n_ens)
        pltpu.make_async_remote_copy(
            src_ref=sc.at[other], dst_ref=sc.at[other], send_sem=sc_send.at[k], recv_sem=sc_recv.at[other],
            device_id={"ens": other}, device_id_type=MESH,
        ).wait_recv()
    scores = sc[0]
    for k in range(1, n_ens):
        scores += sc[k]
    row = lax.broadcasted_iota(jnp.int32, (lines, docs), 0)
    cutoff = jnp.zeros((lines, docs), jnp.float32)
    mean_cutoff = jnp.float32(0.0)
    for m in range(members):
        level = thr_ref[m].astype(jnp.float32) * (1.0 / 256.0)
        cutoff = jnp.where(row == m, level, cutoff)
        mean_cutoff += level * (1.0 / members)
    kept = mask_ref[...].reshape(1, docs).astype(jnp.float32) * jax.nn.sigmoid(4.0 * (scores - cutoff))
    ens_score = jnp.sum(scores, axis=0, keepdims=True) * (1.0 / members)
    ens_kept = jax.nn.sigmoid(4.0 * (ens_score - mean_cutoff))
    kept_sum = jnp.sum(kept, axis=1, keepdims=True)
    agree_sum = jnp.sum(kept * ens_kept, axis=1, keepdims=True)
    lane = lax.broadcasted_iota(jnp.int32, (lines, 128), 1)
    tot[me] = jnp.where(lane == 0, kept_sum, jnp.where(lane == 1, agree_sum, 0.0))

    def tot_copy(k):
        return pltpu.make_async_remote_copy(
            src_ref=tot.at[me], dst_ref=tot.at[me], send_sem=tot_send.at[k], recv_sem=tot_recv.at[me],
            device_id={"dp": lax.rem(me + k, n_dp)}, device_id_type=MESH,
        )

    for k in range(1, n_dp):
        tot_copy(k).start()

    for b in range(PARTS):
        piece = pl.ds(b * (docs // PARTS), docs // PARTS)
        for k in range(1, n_ens):
            other = lax.rem(ens + k, n_ens)
            block = part.at[other, piece, :]
            pltpu.make_async_remote_copy(
                src_ref=block, dst_ref=block, send_sem=part_send.at[k, b], recv_sem=part_recv.at[other, b],
                device_id={"ens": other}, device_id_type=MESH,
            ).wait_recv()
        total = part[0, piece, :].astype(jnp.float32)
        for k in range(1, n_ens):
            total += part[k, piece, :].astype(jnp.float32)
        out_ref[piece, :] = total

    for k in range(1, n_dp):
        other = lax.rem(me + k, n_dp)
        pltpu.make_async_remote_copy(
            src_ref=tot.at[other], dst_ref=tot.at[other], send_sem=tot_send.at[k], recv_sem=tot_recv.at[other],
            device_id={"dp": other}, device_id_type=MESH,
        ).wait_recv()
    sums = tot[0]
    for k in range(1, n_dp):
        sums += tot[k]
    sums = sums / docs
    own = members // n_ens
    row = lax.broadcasted_iota(jnp.int32, (lines, 128), 0)
    for j in range(own):
        mine = row == ens * own + j
        kept_ref[j] = jnp.sum(jnp.where(mine & (lane == 0), sums, 0.0))
        agree_ref[j] = jnp.sum(jnp.where(mine & (lane == 1), sums, 0.0))

    for k in range(n_chips):
        zo, xo = place_of(k)
        for c in range(max(0, chunks - slots), chunks):
            for i, d in enumerate(dirs):
                @pl.when(goes(d, jnp.int32(c), zo, xo))
                def _():
                    sending(i, d, jnp.int32(c), zo, xo).wait_send()
    for k in range(1, n_ens):
        sc_copy(k).wait_send()
        for b in range(PARTS):
            part_copy(k, b).wait_send()
    for k in range(1, n_dp):
        tot_copy(k).wait_send()


def solution(mesh):
    geo = geometry(mesh)
    nz, nx, nc = geo
    n_dp, n_ens = mesh.shape["dp"], mesh.shape["ens"]

    def on_device(embeddings, valid_mask, first_weight, second_weight, thresholds):
        docs, width = embeddings.shape
        members, rows, units = first_weight.shape
        classes = second_weight.shape[2]
        chunks = members * units // COLS
        own = members // n_ens
        lines = -(-members // 8) * 8
        dma = pltpu.SemaphoreType.DMA
        hbm, vmem, smem = (pl.BlockSpec(memory_space=s) for s in (pl.ANY, pltpu.VMEM, pltpu.SMEM))
        return pl.pallas_call(
            functools.partial(kernel, geo, n_ens),
            out_shape=(
                jax.ShapeDtypeStruct((docs, classes), jnp.float32),
                jax.ShapeDtypeStruct((own,), jnp.float32),
                jax.ShapeDtypeStruct((own,), jnp.float32),
            ),
            in_specs=[hbm, vmem, hbm, hbm, smem],
            out_specs=(vmem, smem, smem),
            scratch_shapes=[
                pltpu.VMEM((chunks, width, COLS), jnp.bfloat16),
                pltpu.VMEM((docs, width), jnp.bfloat16),
                pltpu.VMEM(second_weight.shape, jnp.bfloat16),
                pltpu.VMEM((members, docs, classes), jnp.float32),
                pltpu.VMEM((n_ens, docs, classes), jnp.bfloat16),
                pltpu.VMEM((n_ens, lines, docs), jnp.float32),
                pltpu.VMEM((n_dp, lines, 128), jnp.float32),
                dma((chunks,)),
                dma((2,)),
                dma((SLOTS, 4 + nc - 1, nz * nx)),
                dma((chunks, n_dp)),
                dma((n_ens, PARTS)),
                dma((n_ens, PARTS)),
                dma((n_ens,)),
                dma((n_ens,)),
                dma((n_dp,)),
                dma((n_dp,)),
            ],
            compiler_params=pltpu.CompilerParams(
                collective_id=0, has_side_effects=True, vmem_limit_bytes=63 * 1024 * 1024
            ),
        )(embeddings, valid_mask, first_weight, second_weight, thresholds)

    return jax.shard_map(
        on_device,
        mesh=mesh,
        in_specs=(P("dp", None), P("dp"), P(None, "dp", "ens"), P(None, "ens", None), P()),
        out_specs=(P("dp", None), P("ens"), P("ens")),
        check_vma=False,
    )
```

```python
import functools

import jax
import jax.numpy as jnp
from jax import lax
from jax.experimental import pallas as pl
from jax.experimental.pallas import tpu as pltpu
from jax.sharding import PartitionSpec as P

MESH = pl.DeviceIdType.MESH
COLS = 512
LAG = 2
PARTS = 2
SLOTS = 2


def geometry(mesh):
    line = [tuple(d.coords) for d in mesh.devices.reshape(mesh.devices.shape[0], -1)[:, 0]]
    cores = sum(c == line[0] for c in line)
    chips = line[::cores]
    inner = 1
    if len(chips) > 1:
        axis = [a != b for a, b in zip(chips[0], chips[1])].index(True)
        while inner < len(chips) and chips[inner][axis] == chips[0][axis] + inner:
            inner += 1
    return len(chips) // inner, inner, cores


def turned_period(nz, nx):
    even = (nz - 1) * nx - (nx - 1)
    slope = (nz - 1) * (nx - 1) + (nz - 1) * (nx - 1)
    share = 1.0 - even / slope if slope else 0.0
    return round(1 / share) if share > 0 else 0


def kernel(
    geo, n_ens, emb_hbm, mask_ref, fw_hbm, sw_hbm, thr_ref, out_ref, kept_ref, agree_ref,
    w, emb, sw, acc, part, sc, tot,
    local_sem, emb_sem, send_sem, recv_sem, part_send, part_recv, sc_send, sc_recv, tot_sem, core_send, core_recv,
):
    nz, nx, nc = geo
    n_dp = nz * nx * nc
    n_chips = nz * nx
    members, rows, units = fw_hbm.shape
    per_member = units // COLS
    chunks = members * per_member
    docs, classes = out_ref.shape
    period = turned_period(nz, nx)
    reach = nz - 1 + nx - 1
    slots = send_sem.shape[0]

    me = lax.axis_index("dp")
    ens = lax.axis_index("ens")
    core = lax.rem(me, nc)
    chip = me // nc
    z, x = chip // nx, lax.rem(chip, nx)

    def origin_rows(origin):
        return pl.ds(pl.multiple_of(origin * rows, rows), rows)

    def own_copy(c):
        cols = pl.ds(pl.multiple_of(lax.rem(c, per_member) * COLS, COLS), COLS)
        return pltpu.make_async_copy(
            fw_hbm.at[c // per_member, :, cols], w.at[c, origin_rows(me), :], local_sem.at[c]
        )

    for c in range(chunks):
        own_copy(jnp.int32(c)).start()
    emb_copy = pltpu.make_async_copy(emb_hbm, emb, emb_sem.at[0])
    sw_copy = pltpu.make_async_copy(sw_hbm, sw, emb_sem.at[1])
    emb_copy.start()
    sw_copy.start()

    barrier = pltpu.get_barrier_semaphore()
    dirs = []
    if nz > 1:
        dirs += [("z", 1), ("z", -1)]
    if nx > 1:
        dirs += [("x", 1), ("x", -1)]
    dirs += [("c", k) for k in range(1, nc)]

    def target(d):
        kind, k = d
        if kind == "z":
            return me + k * nx * nc
        if kind == "x":
            return me + k * nc
        return chip * nc + lax.rem(core + k, nc)

    def there(d):
        kind, k = d
        if kind == "c":
            return None
        at, n = (z, nz) if kind == "z" else (x, nx)
        return at + 1 < n if k > 0 else at > 0

    waits = jnp.int32(nc - 1 + n_ens - 1)
    for d in dirs:
        ok = there(d)
        if ok is None:
            pl.semaphore_signal(barrier, inc=1, device_id={"dp": target(d)}, device_id_type=MESH)
        else:
            @pl.when(ok)
            def _():
                pl.semaphore_signal(barrier, inc=1, device_id={"dp": target(d)}, device_id_type=MESH)
            waits = waits + ok.astype(jnp.int32)
    for k in range(1, n_ens):
        pl.semaphore_signal(
            barrier, inc=1, device_id={"ens": lax.rem(ens + k, n_ens)}, device_id_type=MESH
        )
    pl.semaphore_wait(barrier, waits)

    def turned(c):
        if not period:
            return jnp.bool_(False)
        return lax.rem(c * nc + core, period) == period // 2

    def goes(d, c, zo, xo):
        kind, k = d
        if kind == "c":
            return c >= 0
        inner_first = turned(c)
        if kind == "z":
            away = (z >= zo) if k > 0 else (z <= zo)
            return away & there(d) & ((xo == x) | inner_first)
        away = (x >= xo) if k > 0 else (x <= xo)
        return away & there(d) & ((zo == z) | jnp.logical_not(inner_first))

    def sending(i, d, c, zo, xo):
        place = zo * nx + xo
        origin = place * nc + core
        block = w.at[c, origin_rows(origin), :]
        if d[0] == "c":
            sems = core_send.at[c, d[1]], core_recv.at[c, d[1]]
        else:
            sems = send_sem.at[lax.rem(c, slots), i, place], recv_sem.at[c, place]
        return pltpu.make_async_remote_copy(
            src_ref=block, dst_ref=block, send_sem=sems[0], recv_sem=sems[1],
            device_id={"dp": target(d)}, device_id_type=MESH,
        )

    def from_cores(c, k):
        blocks = w.at[c, pl.ds(0, n_chips * rows), :]
        return pltpu.make_async_remote_copy(
            src_ref=blocks, dst_ref=blocks,
            send_sem=core_send.at[c, k], recv_sem=core_recv.at[c, k],
            device_id={"dp": target(("c", k))}, device_id_type=MESH,
        )

    def arrived(c, place):
        block = w.at[c, origin_rows(place * nc + core), :]
        pltpu.make_async_remote_copy(
            src_ref=block, dst_ref=block, send_sem=send_sem.at[0, 0, 0], recv_sem=recv_sem.at[c, place],
            device_id={"dp": target(dirs[-1])}, device_id_type=MESH,
        ).wait_recv()

    def place_of(k):
        kz, kx = divmod(k, nx)
        return lax.rem(z + kz, nz), lax.rem(x + kx, nx)

    acc[...] = jnp.zeros_like(acc)

    def compute(done):
        @pl.when(done >= 0)
        def _():
            @pl.when(done == 0)
            def _():
                emb_copy.wait()
                sw_copy.wait()
            for o in range(1, nc):
                from_cores(done, o).wait_recv()
            m = done // per_member
            cols = pl.ds(pl.multiple_of(lax.rem(done, per_member) * COLS, COLS), COLS)
            hidden = jnp.maximum(
                jnp.dot(emb[...], w[done], preferred_element_type=jnp.float32), 0.0
            ).astype(jnp.bfloat16)
            acc[m] += jnp.dot(hidden, sw[m, cols, :], preferred_element_type=jnp.float32)

    def step(t, carry):
        for k in range(n_chips):
            zo, xo = place_of(k)
            c = t - LAG * (jnp.abs(z - zo) + jnp.abs(x - xo))

            @pl.when((c >= 0) & (c < chunks))
            def _():
                if k == 0:
                    own_copy(c).wait()
                else:
                    arrived(c, zo * nx + xo)
                for i, d in enumerate(dirs):
                    if d[0] == "c":
                        sending(i, d, c, zo, xo).start()
                        continue

                    @pl.when((c >= slots) & goes(d, c - slots, zo, xo))
                    def _():
                        sending(i, d, c - slots, zo, xo).wait_send()

                    @pl.when(goes(d, c, zo, xo))
                    def _():
                        sending(i, d, c, zo, xo).start()

            if k == n_chips - 1:
                compute(t - LAG * reach - 1)
        return carry

    lax.fori_loop(0, chunks + LAG * reach + 1, step, 0)

    lines = sc.shape[1]
    levels = lax.broadcasted_iota(jnp.int32, (lines, classes), 1).astype(jnp.float32)
    grades = (2.0 * levels / (classes - 1) - 1.0) * jnp.sqrt(jnp.float32(3.0 / classes))
    line = lax.broadcasted_iota(jnp.int32, (lines, classes), 0)
    own_scores = jnp.zeros((lines, docs), jnp.float32)
    for m in range(members):
        own_scores += lax.dot_general(
            jnp.where(line == m, grades, 0.0), acc[m], (((1,), (1,)), ((), ())),
            precision=lax.Precision.HIGHEST, preferred_element_type=jnp.float32,
        )
    sc[ens] = own_scores

    def sc_copy(k):
        return pltpu.make_async_remote_copy(
            src_ref=sc.at[ens], dst_ref=sc.at[ens], send_sem=sc_send.at[k], recv_sem=sc_recv.at[ens],
            device_id={"ens": lax.rem(ens + k, n_ens)}, device_id_type=MESH,
        )

    def part_copy(k, b):
        piece = part.at[ens, pl.ds(b * (docs // PARTS), docs // PARTS), :]
        return pltpu.make_async_remote_copy(
            src_ref=piece, dst_ref=piece, send_sem=part_send.at[k, b], recv_sem=part_recv.at[ens, b],
            device_id={"ens": lax.rem(ens + k, n_ens)}, device_id_type=MESH,
        )

    for k in range(1, n_ens):
        sc_copy(k).start()
    for b in range(PARTS):
        piece = pl.ds(b * (docs // PARTS), docs // PARTS)
        total = acc[0, piece, :]
        for m in range(1, members):
            total += acc[m, piece, :]
        part[ens, piece, :] = (total * (1.0 / members)).astype(jnp.bfloat16)
        for k in range(1, n_ens):
            part_copy(k, b).start()

    for k in range(1, n_ens):
        other = lax.rem(ens + k, n_ens)
        pltpu.make_async_remote_copy(
            src_ref=sc.at[other], dst_ref=sc.at[other], send_sem=sc_send.at[k], recv_sem=sc_recv.at[other],
            device_id={"ens": other}, device_id_type=MESH,
        ).wait_recv()
    scores = sc[0]
    for k in range(1, n_ens):
        scores += sc[k]
    row = lax.broadcasted_iota(jnp.int32, (lines, docs), 0)
    cutoff = jnp.zeros((lines, docs), jnp.float32)
    mean_cutoff = jnp.float32(0.0)
    for m in range(members):
        level = thr_ref[m].astype(jnp.float32) * (1.0 / 256.0)
        cutoff = jnp.where(row == m, level, cutoff)
        mean_cutoff += level * (1.0 / members)
    kept = mask_ref[...].reshape(1, docs).astype(jnp.float32) * jax.nn.sigmoid(4.0 * (scores - cutoff))
    ens_score = jnp.sum(scores, axis=0, keepdims=True) * (1.0 / members)
    ens_kept = jax.nn.sigmoid(4.0 * (ens_score - mean_cutoff))
    kept_sum = jnp.sum(kept, axis=1, keepdims=True)
    agree_sum = jnp.sum(kept * ens_kept, axis=1, keepdims=True)
    lane = lax.broadcasted_iota(jnp.int32, (lines, 128), 1)
    tot[me] = jnp.where(lane == 0, kept_sum, jnp.where(lane == 1, agree_sum, 0.0))

    def tot_copy(k):
        return pltpu.make_async_remote_copy(
            src_ref=tot.at[me], dst_ref=tot.at[me], send_sem=tot_sem.at[0], recv_sem=tot_sem.at[1],
            device_id={"dp": lax.rem(me + k, n_dp)}, device_id_type=MESH,
        )

    tiles = tot.at[pl.ds(0, n_dp - 1)]
    all_tot = pltpu.make_async_remote_copy(
        src_ref=tiles, dst_ref=tiles, send_sem=tot_sem.at[0], recv_sem=tot_sem.at[1],
        device_id={"dp": lax.rem(me + 1, n_dp)}, device_id_type=MESH,
    )

    for k in range(1, n_dp):
        tot_copy(k).start()

    for b in range(PARTS):
        piece = pl.ds(b * (docs // PARTS), docs // PARTS)
        for k in range(1, n_ens):
            other = lax.rem(ens + k, n_ens)
            block = part.at[other, piece, :]
            pltpu.make_async_remote_copy(
                src_ref=block, dst_ref=block, send_sem=part_send.at[k, b], recv_sem=part_recv.at[other, b],
                device_id={"ens": other}, device_id_type=MESH,
            ).wait_recv()
        total = part[0, piece, :].astype(jnp.float32)
        for k in range(1, n_ens):
            total += part[k, piece, :].astype(jnp.float32)
        out_ref[piece, :] = total

    all_tot.wait_recv()
    sums = tot[0]
    for k in range(1, n_dp):
        sums += tot[k]
    sums = sums / docs
    own = members // n_ens
    row = lax.broadcasted_iota(jnp.int32, (lines, 128), 0)
    for j in range(own):
        mine = row == ens * own + j
        kept_ref[j] = jnp.sum(jnp.where(mine & (lane == 0), sums, 0.0))
        agree_ref[j] = jnp.sum(jnp.where(mine & (lane == 1), sums, 0.0))

    for k in range(n_chips):
        zo, xo = place_of(k)
        for c in range(max(0, chunks - slots), chunks):
            for i, d in enumerate(dirs):
                if d[0] != "c":
                    @pl.when(goes(d, jnp.int32(c), zo, xo))
                    def _():
                        sending(i, d, jnp.int32(c), zo, xo).wait_send()
    for c in range(chunks):
        for k in range(1, nc):
            from_cores(c, k).wait_send()
    for k in range(1, n_ens):
        sc_copy(k).wait_send()
        for b in range(PARTS):
            part_copy(k, b).wait_send()
    all_tot.wait_send()


def solution(mesh):
    geo = geometry(mesh)
    nz, nx, nc = geo
    n_dp, n_ens = mesh.shape["dp"], mesh.shape["ens"]

    def on_device(embeddings, valid_mask, first_weight, second_weight, thresholds):
        docs, width = embeddings.shape
        members, rows, units = first_weight.shape
        classes = second_weight.shape[2]
        chunks = members * units // COLS
        own = members // n_ens
        lines = -(-members // 8) * 8
        dma = pltpu.SemaphoreType.DMA
        hbm, vmem, smem = (pl.BlockSpec(memory_space=s) for s in (pl.ANY, pltpu.VMEM, pltpu.SMEM))
        return pl.pallas_call(
            functools.partial(kernel, geo, n_ens),
            out_shape=(
                jax.ShapeDtypeStruct((docs, classes), jnp.float32),
                jax.ShapeDtypeStruct((own,), jnp.float32),
                jax.ShapeDtypeStruct((own,), jnp.float32),
            ),
            in_specs=[hbm, vmem, hbm, hbm, smem],
            out_specs=(vmem, smem, smem),
            scratch_shapes=[
                pltpu.VMEM((chunks, width, COLS), jnp.bfloat16),
                pltpu.VMEM((docs, width), jnp.bfloat16),
                pltpu.VMEM(second_weight.shape, jnp.bfloat16),
                pltpu.VMEM((members, docs, classes), jnp.float32),
                pltpu.VMEM((n_ens, docs, classes), jnp.bfloat16),
                pltpu.VMEM((n_ens, lines, docs), jnp.float32),
                pltpu.VMEM((n_dp, lines, 128), jnp.float32),
                dma((chunks,)),
                dma((2,)),
                dma((SLOTS, 4, nz * nx)),
                dma((chunks, nz * nx)),
                dma((n_ens, PARTS)),
                dma((n_ens, PARTS)),
                dma((n_ens,)),
                dma((n_ens,)),
                dma((2,)),
                dma((chunks, nc)),
                dma((chunks, nc)),
            ],
            compiler_params=pltpu.CompilerParams(
                collective_id=0, has_side_effects=True, vmem_limit_bytes=63 * 1024 * 1024
            ),
        )(embeddings, valid_mask, first_weight, second_weight, thresholds)

    return jax.shard_map(
        on_device,
        mesh=mesh,
        in_specs=(P("dp", None), P("dp"), P(None, "dp", "ens"), P(None, "ens", None), P()),
        out_specs=(P("dp", None), P("ens"), P("ens")),
        check_vma=False,
    )
```
